32 devices in a mesh: row: 8 (over z, core), col: 4 (over y, x).
Axes of the slice: x: 2, y: 2, z: 4, core: 2. Of those that a mesh axis runs over, the one named last changes fastest.
Arguments:
- wrapped_phase: float32 [16384, 2048], P('row', 'col'), may hold values from -2.85 to 2.85, as said below
Outputs:
- unwrapped: float32 [16384, 2048], P('row', 'col')
The draws below stay inside these ranges and needn't reach their ends.
Inputs may be any that keep to these rules, and one draw needn't show every extreme that they name: The difference of wrapped_phase between any two adjacent cells of the map lies 0.14 or more away from every odd multiple of pi.
All inputs are finite; a program needn't handle non-finite values.
Results may differ from the reference program's by a relative error of at most 0.0003.
Values sent between devices are 32-bit elements; how exact they have to be, the bound alone decides.
A program may use at most 128 MiB of HBM per device.

```python
import math
import jax
import jax.numpy as jnp
from jax import lax

TILE = 256
NX = 16384
NY = 2048


def draw_wrapped_phase(key, part):
    keys = jax.random.split(jax.random.fold_in(key, 11), 5)
    row_index = jnp.arange(NX, dtype=jnp.int32)[:, None]
    col_index = jnp.arange(NY, dtype=jnp.int32)[None, :]
    rates = jax.random.randint(keys[0], (2, 2), 1, 17)
    periods = jax.random.randint(keys[1], (2,), 2, 5)
    anchors = jax.random.randint(keys[2], (2,), 0, 64)
    levels = jnp.zeros((NX, NY), jnp.int32)
    for mode in range(2):
        position = (row_index * rates[mode, 0] + col_index * rates[mode, 1]) // 16 + anchors[mode]
        cycle = jnp.remainder(position, 2 * periods[mode])
        levels = levels + jnp.abs(cycle - periods[mode])
    levels = levels + jax.random.randint(keys[3], (NX, NY), 0, 4)
    centred = jnp.remainder(levels, 7) - 3
    jitter = jax.random.uniform(keys[4], (NX, NY), jnp.float32, -0.149, 0.149)
    return centred.astype(jnp.float32) * (2.0 * math.pi / 7.0) + jitter


def setup_inputs(seed: int = 0) -> dict:
    splits = jax.random.split(jax.random.key(seed), 2)
    wrapped_phase = draw_wrapped_phase(jax.random.fold_in(splits[1], 71), 0)
    return dict(wrapped_phase=wrapped_phase)


HIGHEST = lax.Precision.HIGHEST

def wrap_angle(values):
    return jnp.arctan2(jnp.sin(values), jnp.cos(values))

def cosine_table(length):
    frequency = jnp.arange(length, dtype=jnp.float32)[:, None]
    positions = jnp.arange(length, dtype=jnp.float32)[None, :]
    cosine = jnp.cos(math.pi * frequency * (2.0 * positions + 1.0) / (2.0 * length)) * math.sqrt(2.0 / length)
    return jnp.where(frequency == 0.0, cosine * math.sqrt(0.5), cosine)

def solve_tiles(phase_grid):
    length = phase_grid.shape[1]
    down_slope = wrap_angle(phase_grid[:, 1:] - phase_grid[:, :-1])
    zero_row = jnp.zeros_like(phase_grid[:, :1])
    diverge = jnp.concatenate([down_slope, zero_row], 1) - jnp.concatenate([zero_row, down_slope], 1)
    across = wrap_angle(phase_grid[..., 1:] - phase_grid[..., :-1])
    zero_col = jnp.zeros_like(phase_grid[..., :1])
    diverge = diverge + jnp.concatenate([across, zero_col], 3) - jnp.concatenate([zero_col, across], 3)
    cosine = cosine_table(length)
    spectrum = jnp.einsum('pa,rakb,qb->rpkq', cosine, diverge, cosine, precision=HIGHEST)
    frequency = jnp.arange(length, dtype=jnp.float32)
    wave_cos = 2.0 * jnp.cos(math.pi * frequency / length)
    eigenvalue = wave_cos[:, None] + wave_cos[None, :] - 4.0
    corner = frequency[:, None] + frequency[None, :] == 0.0
    safe_eigen = jnp.where(corner, -1.0, eigenvalue)
    scaled = jnp.where(corner[:, None, :], 0.0, spectrum / safe_eigen[:, None, :])
    return jnp.einsum('pa,rpkq,qb->rakb', cosine, scaled, cosine, precision=HIGHEST)

def reference(wrapped_phase):
    tile_rows = NX // TILE
    tile_cols = NY // TILE
    phase_grid = wrapped_phase.reshape(tile_rows, TILE, tile_cols, TILE)
    solved = lax.map(lambda band_tiles: solve_tiles(band_tiles[None])[0], phase_grid)
    east_jump = lax.optimization_barrier(jnp.mean(solved[:, :, :-1, -1] + wrap_angle(phase_grid[:, :, 1:, 0] - phase_grid[:, :, :-1, -1]) - solved[:, :, 1:, 0], axis=1))
    south_jump = lax.optimization_barrier(jnp.mean(solved[:-1, -1, 0, :] + wrap_angle(phase_grid[1:, 0, 0, :] - phase_grid[:-1, -1, 0, :]) - solved[1:, 0, 0, :], axis=1))
    row_starts = jnp.concatenate([jnp.zeros((1,), jnp.float32), jnp.cumsum(south_jump)])
    along_row = jnp.concatenate([jnp.zeros((tile_rows, 1), jnp.float32), jnp.cumsum(east_jump, axis=1)], 1)
    offsets = row_starts[:, None] + along_row
    return (solved + offsets[:, None, :, None]).reshape(NX, NY)
```

```python
import functools
import math

import jax
import jax.numpy as jnp
import numpy as np
from jax import lax
from jax.experimental import pallas as pl
from jax.experimental.pallas import tpu as pltpu
from jax.sharding import PartitionSpec as P

TILE = 256
FULL_TURN = 2.0 * math.pi
MESH = pl.DeviceIdType.MESH
LANES = 128


def wrap_angle(values):
    return values - FULL_TURN * jnp.floor(values * (1.0 / FULL_TURN) + 0.5)


def cos32(angle):
    return np.cos(angle.astype(np.float64)).astype(np.float32)


def tables(length):
    f32 = np.float32
    order = np.arange(length, dtype=f32)
    angle = (f32(math.pi) * order)[:, None] * (f32(2) * order + f32(1))[None, :] / f32(2 * length)
    cosine = cos32(angle) * f32(math.sqrt(2.0 / length))
    cosine[0] = cosine[0] * f32(math.sqrt(0.5))
    wave = f32(2) * cos32(f32(math.pi) * order / f32(length))
    eigen = (wave[:, None] + wave[None, :]) - f32(4)
    eigen[0, 0] = -1
    inverse = 1.0 / eigen.astype(np.float64)
    inverse[0, 0] = 0
    c64 = cosine.astype(np.float64)
    weights = []
    for cell in (length - 1, 0):
        green = (c64[:, cell] * inverse[0]) @ c64
        step = green - np.append(green[1:], 0.0)
        step[-1] = 0
        weights.append(step / length)
    return cosine, inverse.astype(f32), np.stack(weights).astype(f32)


def split(values):
    high = values.astype(jnp.bfloat16)
    low = (values - high.astype(jnp.float32)).astype(jnp.bfloat16)
    return high, low


def dot(left, right):
    return jnp.dot(left, right, preferred_element_type=jnp.float32)


def times_right(values, table):
    high, low = split(values)
    return dot(jnp.concatenate([high, low, high], 1), table)


def times_left(table, values):
    high, low = split(values)
    return dot(table, jnp.concatenate([high, low, high], 0))


def slopes(band):
    rows, width = band.shape
    down = wrap_angle(pltpu.roll(band, rows - 1, 0) - band)
    across = wrap_angle(pltpu.roll(band, width - 1, 1) - band)
    return down, across


def solve_kernel(x_ref, off_ref, left1, right1, left2, right2, inv_ref, out_ref):
    index = pl.program_id(0)
    band = x_ref[...]
    rows, width = band.shape
    down, across = slopes(band)
    row_id = lax.broadcasted_iota(jnp.int32, band.shape, 0)
    col_id = lax.broadcasted_iota(jnp.int32, band.shape, 1) % TILE
    down = jnp.where(row_id == TILE - 1, 0.0, down)
    across = jnp.where(col_id == TILE - 1, 0.0, across)
    diverge = down - pltpu.roll(down, 1, 0) + across - pltpu.roll(across, 1, 1)
    for t in range(width // TILE):
        cols = slice(t * TILE, (t + 1) * TILE)
        inner = times_right(diverge[:, cols], right1[...])
        scaled = times_left(left1[...], inner) * inv_ref[...]
        inner = times_right(scaled, right2[...])
        solved = times_left(left2[...], inner)
        out_ref[:, cols] = solved + off_ref[pl.ds(index, 1), cols]


def lane_sum(values):
    return jnp.sum(values, axis=1, keepdims=True)


def running(values):
    n = values.shape[0]
    row = lax.broadcasted_iota(jnp.int32, values.shape, 0)
    total = jnp.zeros_like(values)
    for k in range(n - 1):
        total = total + jnp.where(row > k, values[k : k + 1], 0.0)
    return total


def chain_kernel(
    n_row, n_col, x_ref, w_ref, off_ref,
    col_out, col_in, top_out, top_in, sum_s, sum_d, first_s, last_s,
    down_out, down_in, row_out, row_in,
    edge_send, edge_recv, down_send, down_recv, row_send, row_recv,
):
    r, c = lax.axis_index("row"), lax.axis_index("col")
    height, width = x_ref.shape
    bands, tiles = height // TILE, width // TILE

    barrier = pltpu.get_barrier_semaphore()
    for k in range(1, n_row):
        pl.semaphore_signal(barrier, inc=1, device_id=(lax.rem(r + k, n_row), c), device_id_type=MESH)
    for k in range(1, n_col):
        pl.semaphore_signal(barrier, inc=1, device_id=(r, lax.rem(c + k, n_col)), device_id_type=MESH)

    for i in range(bands):
        rows = pl.ds(i * TILE, TILE)
        col_out[i : i + 1, :] = jnp.transpose(x_ref[rows, 0:LANES])[0:1, :]
    top_out[...] = jnp.broadcast_to(x_ref[0:1, 0:TILE], top_out.shape)

    pl.semaphore_wait(barrier, n_row + n_col - 2)
    edge_col = pltpu.make_async_remote_copy(
        src_ref=col_out, dst_ref=col_in, send_sem=edge_send.at[0], recv_sem=edge_recv.at[0],
        device_id=(r, lax.rem(c + n_col - 1, n_col)), device_id_type=MESH)
    edge_top = pltpu.make_async_remote_copy(
        src_ref=top_out, dst_ref=top_in, send_sem=edge_send.at[1], recv_sem=edge_recv.at[1],
        device_id=(lax.rem(r + n_row - 1, n_row), c), device_id_type=MESH)
    edge_col.start()
    edge_top.start()

    for i in range(bands):
        rows = pl.ds(i * TILE, TILE)
        band = x_ref[rows, :]
        across = wrap_angle(pltpu.roll(band, width - 1, 1) - band)
        sum_s[i : i + 1, :] = jnp.sum(across, axis=0, keepdims=True)
        first = band[:, 0:TILE]
        down = wrap_angle(pltpu.roll(first, TILE - 1, 0) - first)
        weight = w_ref[:, 2 * TILE : 2 * TILE + 2]
        sum_d[i : i + 1, :] = jnp.sum(down * weight[:, 0:1], axis=0, keepdims=True)
        sum_d[bands + i : bands + i + 1, :] = jnp.sum(down * weight[:, 1:2], axis=0, keepdims=True)
        first_s[i : i + 1, :] = first[0:1, :]
        last_s[i : i + 1, :] = first[TILE - 1 : TILE, :]
        last_col = jnp.transpose(x_ref[rows, width - LANES : width])
        last_s[bands + i : bands + i + 1, :] = last_col[LANES - 1 : LANES, :]

    scale = 1.0 / TILE
    down_last = lane_sum(sum_d[0:bands, :])
    down_first = lane_sum(sum_d[bands : 2 * bands, :])
    edge_top.wait()
    edge_col.wait()
    below = jnp.concatenate([first_s[1:bands, :], top_in[0:1, :]], 0)
    border = lane_sum(wrap_angle(below - last_s[0:bands, :])) * scale
    band_id = lax.broadcasted_iota(jnp.int32, (bands, 1), 0)
    next_first = jnp.concatenate([down_first[1:bands], down_first[0:1]], 0)
    jump = down_last + border - next_first
    jump_total = jnp.sum(jump, axis=0, keepdims=True)
    starts = running(jump)
    lane = lax.broadcasted_iota(jnp.int32, (8, LANES), 1)
    down_first0 = down_first[0:1]
    down_out[...] = jnp.where(lane == 0, jump_total, jnp.where(lane == 1, down_first0, 0.0))
    copies = []
    for k in range(1, n_row):
        copies.append(pltpu.make_async_remote_copy(
            src_ref=down_out, dst_ref=down_in.at[k - 1],
            send_sem=down_send.at[k - 1], recv_sem=down_recv.at[k - 1],
            device_id=(lax.rem(r + k, n_row), c), device_id_type=MESH))
    for copy in copies:
        copy.start()

    sums = sum_s[...]
    last_w, first_w = w_ref[0:1, 0:TILE], w_ref[0:1, TILE : 2 * TILE]
    lasts = [lane_sum(sums[:, t * TILE : (t + 1) * TILE] * last_w) for t in range(tiles)]
    firsts = [lane_sum(sums[:, t * TILE : (t + 1) * TILE] * first_w) for t in range(tiles)]
    along = [jnp.zeros((bands, 1), jnp.float32)]
    for t in range(tiles - 1):
        end = (t + 1) * TILE
        along.append(along[-1] + lasts[t] + sums[:, end - 1 : end] * scale - firsts[t + 1])
    edge = lane_sum(wrap_angle(col_in[...] - last_s[bands : 2 * bands, :])) * scale
    row_total = along[-1] + lasts[-1] + edge - firsts[0]

    for copy in copies:
        copy.wait()
    above = jnp.zeros((1, 1), jnp.float32)
    origin = jnp.where(r == 0, down_first0, 0.0)
    for k in range(1, n_row):
        got = down_in[k - 1]
        above = above + jnp.where(k <= r, got[0:1, 0:1], 0.0)
        origin = origin + jnp.where(k == r, got[0:1, 1:2], 0.0)
    starts = starts + above + origin - down_first0

    lane = lax.broadcasted_iota(jnp.int32, (bands, LANES), 1)
    row_out[...] = jnp.where(
        lane == 0, row_total, jnp.where(lane == 1, starts + firsts[0], 0.0))
    copies = []
    for k in range(1, n_col):
        copies.append(pltpu.make_async_remote_copy(
            src_ref=row_out, dst_ref=row_in.at[k - 1],
            send_sem=row_send.at[k - 1], recv_sem=row_recv.at[k - 1],
            device_id=(r, lax.rem(c + k, n_col)), device_id_type=MESH))
    for copy in copies:
        copy.start()
    for copy in copies:
        copy.wait()
    offset = jnp.where(c == 0, starts + firsts[0], 0.0) - firsts[0]
    for k in range(1, n_col):
        got = row_in[k - 1]
        offset = offset + jnp.where(k <= c, got[:, 0:1], 0.0)
        offset = offset + jnp.where(k == c, got[:, 1:2], 0.0)
    for t in range(tiles):
        off_ref[:, t * TILE : (t + 1) * TILE] = jnp.broadcast_to(offset + along[t], (bands, TILE))


def per_device(n_row, n_col, x):
    height, width = x.shape
    bands = height // TILE
    cosine, inverse, weights = tables(TILE)
    high = cosine.astype(jnp.bfloat16)
    low = (cosine - high.astype(np.float32)).astype(jnp.bfloat16)
    across = lambda h, l: np.concatenate([h, h, l], 1)
    along = lambda h, l: np.concatenate([h, h, l], 0)
    left1, right1 = across(high, low), along(high.T, low.T)
    left2, right2 = across(high.T, low.T), along(high, low)
    w = np.zeros((TILE, 2 * TILE + LANES), np.float32)
    w[:, 0:TILE] = weights[0]
    w[:, TILE : 2 * TILE] = weights[1]
    w[:, 2 * TILE] = weights[0]
    w[:, 2 * TILE + 1] = weights[1]

    vmem = pl.BlockSpec(memory_space=pltpu.VMEM)
    f32 = jnp.float32
    offsets = pl.pallas_call(
        functools.partial(chain_kernel, n_row, n_col),
        out_shape=jax.ShapeDtypeStruct((bands, width), f32),
        in_specs=[vmem, vmem],
        out_specs=vmem,
        scratch_shapes=[
            pltpu.VMEM((bands, TILE), f32),
            pltpu.VMEM((bands, TILE), f32),
            pltpu.VMEM((8, TILE), f32),
            pltpu.VMEM((8, TILE), f32),
            pltpu.VMEM((bands, width), f32),
            pltpu.VMEM((2 * bands, TILE), f32),
            pltpu.VMEM((bands, TILE), f32),
            pltpu.VMEM((2 * bands, TILE), f32),
            pltpu.VMEM((8, LANES), f32),
            pltpu.VMEM((n_row - 1, 8, LANES), f32),
            pltpu.VMEM((bands, LANES), f32),
            pltpu.VMEM((n_col - 1, bands, LANES), f32),
            pltpu.SemaphoreType.DMA((2,)),
            pltpu.SemaphoreType.DMA((2,)),
            pltpu.SemaphoreType.DMA((n_row - 1,)),
            pltpu.SemaphoreType.DMA((n_row - 1,)),
            pltpu.SemaphoreType.DMA((n_col - 1,)),
            pltpu.SemaphoreType.DMA((n_col - 1,)),
        ],
        compiler_params=pltpu.CompilerParams(collective_id=0, has_side_effects=True),
        name="chain",
    )(x, jnp.asarray(w))

    whole = lambda a: pl.BlockSpec(a.shape, lambda i: (0,) * len(a.shape))
    consts = [jnp.asarray(a) for a in (left1, right1, left2, right2, inverse)]
    return pl.pallas_call(
        solve_kernel,
        grid=(bands,),
        out_shape=jax.ShapeDtypeStruct(x.shape, f32),
        in_specs=[pl.BlockSpec((TILE, width), lambda i: (i, 0)), whole(offsets)]
        + [whole(a) for a in consts],
        out_specs=pl.BlockSpec((TILE, width), lambda i: (i, 0)),
        compiler_params=pltpu.CompilerParams(dimension_semantics=("arbitrary",)),
        name="solve",
    )(x, offsets, *consts)


def solution(mesh):
    n_row, n_col = mesh.shape["row"], mesh.shape["col"]
    return jax.shard_map(
        functools.partial(per_device, n_row, n_col), mesh=mesh,
        in_specs=(P("row", "col"),), out_specs=P("row", "col"), check_vma=False,
    )
```

```python
import functools
import math

import jax
import jax.numpy as jnp
import numpy as np
from jax import lax
from jax.experimental import pallas as pl
from jax.experimental.pallas import tpu as pltpu
from jax.sharding import PartitionSpec as P

TILE = 256
FULL_TURN = 2.0 * math.pi
MESH = pl.DeviceIdType.MESH
LANES = 128


def wrap_angle(values):
    return values - FULL_TURN * jnp.floor(values * (1.0 / FULL_TURN) + 0.5)


def cos32(angle):
    return np.cos(angle.astype(np.float64)).astype(np.float32)


def tables(length):
    f32 = np.float32
    order = np.arange(length, dtype=f32)
    angle = (f32(math.pi) * order)[:, None] * (f32(2) * order + f32(1))[None, :] / f32(2 * length)
    cosine = cos32(angle) * f32(math.sqrt(2.0 / length))
    cosine[0] = cosine[0] * f32(math.sqrt(0.5))
    wave = f32(2) * cos32(f32(math.pi) * order / f32(length))
    eigen = (wave[:, None] + wave[None, :]) - f32(4)
    eigen[0, 0] = -1
    inverse = 1.0 / eigen.astype(np.float64)
    inverse[0, 0] = 0
    c64 = cosine.astype(np.float64)
    weights = []
    for cell in (length - 1, 0):
        green = (c64[:, cell] * inverse[0]) @ c64
        step = green - np.append(green[1:], 0.0)
        step[-1] = 0
        weights.append(step / length)
    return cosine, inverse.astype(f32), np.stack(weights).astype(f32)


def split(values):
    high = values.astype(jnp.bfloat16)
    low = (values - high.astype(jnp.float32)).astype(jnp.bfloat16)
    return high, low


def dot(left, right):
    return jnp.dot(left, right, preferred_element_type=jnp.float32)


def stack3(high, low, axis):
    return jnp.concatenate([high, low, high], axis)


def sandwich(high, low, right, left):
    n = high.shape[0]
    table = right[...]
    inner = dot(stack3(high, low, 1), jnp.concatenate([table[:n], table], 0))
    high, low = split(inner)
    table = left[...]
    return dot(jnp.concatenate([table[:, :n], table], 1), stack3(high, low, 0))


def band_rows(i):
    return pl.ds(pl.multiple_of(i * TILE, TILE), TILE)


def band_copy(src, dst, sem, i):
    rows = band_rows(i)
    return pltpu.make_async_copy(src.at[rows, :], dst.at[rows, :], sem.at[i])


def finish_kernel(
    high_hbm, low_hbm, off_ref, left, right, out_hbm, high_s, low_s, out_s, high_sem, low_sem, out_sem
):
    height, width = out_s.shape
    bands, tiles = height // TILE, width // TILE
    for i in range(bands):
        band_copy(high_hbm, high_s, high_sem, i).start()
        band_copy(low_hbm, low_s, low_sem, i).start()

    def step(i, carry):
        rows = band_rows(i)
        band_copy(high_hbm, high_s, high_sem, i).wait()
        band_copy(low_hbm, low_s, low_sem, i).wait()
        for t in range(tiles):
            cols = slice(t * TILE, (t + 1) * TILE)
            solved = sandwich(high_s[rows, cols], low_s[rows, cols], right, left)
            out_s[rows, cols] = solved + off_ref[pl.ds(i, 1), cols]
        band_copy(out_s, out_hbm, out_sem, i).start()
        return carry

    lax.fori_loop(0, bands, step, 0)
    for i in range(bands):
        band_copy(out_s, out_hbm, out_sem, i).wait()


def lane_sum(values):
    return jnp.sum(values, axis=1, keepdims=True)


def running(values):
    n = values.shape[0]
    row = lax.broadcasted_iota(jnp.int32, values.shape, 0)
    total = jnp.zeros_like(values)
    for k in range(n - 1):
        total = total + jnp.where(row > k, values[k : k + 1], 0.0)
    return total


CHUNK = 32


def slope_band(x_s, w_ref, i, bands, dh_s, dl_s, sum_s, sum_d, first_s, last_s):
    width = x_s.shape[1]
    base = pl.multiple_of(i * TILE, TILE)
    shape = (CHUNK, width)
    row_id = lax.broadcasted_iota(jnp.int32, shape, 0)
    tile_end = lax.broadcasted_iota(jnp.int32, shape, 1) % TILE == TILE - 1
    fold = lambda v: jnp.sum(v.reshape(CHUNK // 8, 8, v.shape[1]), axis=0)
    acc = jnp.zeros((8, width), jnp.float32)
    acc_last = jnp.zeros((8, TILE), jnp.float32)
    acc_first = jnp.zeros((8, TILE), jnp.float32)
    before = jnp.zeros((1, width), jnp.float32)
    for k in range(TILE // CHUNK):
        rows = pl.ds(base + k * CHUNK, CHUNK)
        x = x_s[rows, :]
        below = pltpu.roll(x, CHUNK - 1, 0)
        if k < TILE // CHUNK - 1:
            below = jnp.where(row_id == CHUNK - 1, x_s[pl.ds(base + (k + 1) * CHUNK, 1), :], below)
        down = wrap_angle(below - x)
        if k == TILE // CHUNK - 1:
            down = jnp.where(row_id == CHUNK - 1, 0.0, down)
        across = wrap_angle(pltpu.roll(x, width - 1, 1) - x)
        acc = acc + fold(across)
        weight = w_ref[k * CHUNK : (k + 1) * CHUNK, 2 * TILE : 2 * TILE + 2]
        acc_last = acc_last + fold(down[:, :TILE] * weight[:, 0:1])
        acc_first = acc_first + fold(down[:, :TILE] * weight[:, 1:2])
        across = jnp.where(tile_end, 0.0, across)
        above = jnp.where(row_id == 0, before, pltpu.roll(down, 1, 0))
        before = down[CHUNK - 1 : CHUNK, :]
        high, low = split(down - above + across - pltpu.roll(across, 1, 1))
        dh_s[rows, :] = high
        dl_s[rows, :] = low
    sum_s[pl.ds(i, 1), :] = jnp.sum(acc, axis=0, keepdims=True)
    sum_d[pl.ds(i, 1), :] = jnp.sum(acc_last, axis=0, keepdims=True)
    sum_d[pl.ds(bands + i, 1), :] = jnp.sum(acc_first, axis=0, keepdims=True)
    first_s[pl.ds(i, 1), :] = x_s[pl.ds(base, 1), 0:TILE]
    last_s[pl.ds(i, 1), :] = x_s[pl.ds(base + TILE - 1, 1), 0:TILE]


def chain_kernel(
    n_row, n_col, x_hbm, w_ref, left, right, inv_ref, high_hbm, low_hbm, off_ref,
    x_s, dh_s, dl_s, sh_s, sl_s,
    col_out, col_in, top_out, top_in, sum_s, sum_d, first_s, last_s,
    down_out, down_in, row_out, row_in,
    edge_send, edge_recv, down_send, down_recv, row_send, row_recv,
    x_sem, high_sem, low_sem,
):
    r, c = lax.axis_index("row"), lax.axis_index("col")
    height, width = x_s.shape
    bands, tiles = height // TILE, width // TILE
    for i in range(bands):
        band_copy(x_hbm, x_s, x_sem, i).start()

    barrier = pltpu.get_barrier_semaphore()
    for k in range(1, n_row):
        pl.semaphore_signal(barrier, inc=1, device_id=(lax.rem(r + k, n_row), c), device_id_type=MESH)
    for k in range(1, n_col):
        pl.semaphore_signal(barrier, inc=1, device_id=(r, lax.rem(c + k, n_col)), device_id_type=MESH)

    def take_columns(i, carry):
        band_copy(x_hbm, x_s, x_sem, i).wait()
        rows = band_rows(i)
        col_out[pl.ds(i, 1), :] = jnp.transpose(x_s[rows, 0:LANES])[0:1, :]
        ends = jnp.transpose(x_s[rows, width - LANES : width])
        last_s[pl.ds(bands + i, 1), :] = ends[LANES - 1 : LANES, :]
        return carry

    lax.fori_loop(0, bands, take_columns, 0)
    top_out[...] = jnp.broadcast_to(x_s[0:1, 0:TILE], top_out.shape)

    pl.semaphore_wait(barrier, n_row + n_col - 2)
    edge_col = pltpu.make_async_remote_copy(
        src_ref=col_out, dst_ref=col_in, send_sem=edge_send.at[0], recv_sem=edge_recv.at[0],
        device_id=(r, lax.rem(c + n_col - 1, n_col)), device_id_type=MESH)
    edge_top = pltpu.make_async_remote_copy(
        src_ref=top_out, dst_ref=top_in, send_sem=edge_send.at[1], recv_sem=edge_recv.at[1],
        device_id=(lax.rem(r + n_row - 1, n_row), c), device_id_type=MESH)
    edge_col.start()
    edge_top.start()

    def slope_step(i, carry):
        slope_band(x_s, w_ref, i, bands, dh_s, dl_s, sum_s, sum_d, first_s, last_s)
        return carry

    lax.fori_loop(0, bands, slope_step, 0)

    def spectrum_step(i, carry):
        rows = band_rows(i)
        for t in range(tiles):
            cols = slice(t * TILE, (t + 1) * TILE)
            scaled = sandwich(dh_s[rows, cols], dl_s[rows, cols], right, left) * inv_ref[...]
            sh_s[rows, cols], sl_s[rows, cols] = split(scaled)
        band_copy(sh_s, high_hbm, high_sem, i).start()
        band_copy(sl_s, low_hbm, low_sem, i).start()
        return carry

    scale = 1.0 / TILE
    down_last = lane_sum(sum_d[0:bands, :])
    down_first = lane_sum(sum_d[bands : 2 * bands, :])
    edge_top.wait()
    edge_col.wait()
    below = jnp.concatenate([first_s[1:bands, :], top_in[0:1, :]], 0)
    border = lane_sum(wrap_angle(below - last_s[0:bands, :])) * scale
    band_id = lax.broadcasted_iota(jnp.int32, (bands, 1), 0)
    next_first = jnp.concatenate([down_first[1:bands], down_first[0:1]], 0)
    jump = down_last + border - next_first
    jump_total = jnp.sum(jump, axis=0, keepdims=True)
    starts = running(jump)
    lane = lax.broadcasted_iota(jnp.int32, (8, LANES), 1)
    down_first0 = down_first[0:1]
    down_out[...] = jnp.where(lane == 0, jump_total, jnp.where(lane == 1, down_first0, 0.0))
    copies = []
    for k in range(1, n_row):
        copies.append(pltpu.make_async_remote_copy(
            src_ref=down_out, dst_ref=down_in.at[k - 1],
            send_sem=down_send.at[k - 1], recv_sem=down_recv.at[k - 1],
            device_id=(lax.rem(r + k, n_row), c), device_id_type=MESH))
    for copy in copies:
        copy.start()

    sums = sum_s[...]
    last_w, first_w = w_ref[0:1, 0:TILE], w_ref[0:1, TILE : 2 * TILE]
    lasts = [lane_sum(sums[:, t * TILE : (t + 1) * TILE] * last_w) for t in range(tiles)]
    firsts = [lane_sum(sums[:, t * TILE : (t + 1) * TILE] * first_w) for t in range(tiles)]
    along = [jnp.zeros((bands, 1), jnp.float32)]
    for t in range(tiles - 1):
        end = (t + 1) * TILE
        along.append(along[-1] + lasts[t] + sums[:, end - 1 : end] * scale - firsts[t + 1])
    edge = lane_sum(wrap_angle(col_in[...] - last_s[bands : 2 * bands, :])) * scale
    row_total = along[-1] + lasts[-1] + edge - firsts[0]

    lax.fori_loop(0, bands // 2, spectrum_step, 0)
    for copy in copies:
        copy.wait()
    above = jnp.zeros((1, 1), jnp.float32)
    origin = jnp.where(r == 0, down_first0, 0.0)
    for k in range(1, n_row):
        got = down_in[k - 1]
        above = above + jnp.where(k <= r, got[0:1, 0:1], 0.0)
        origin = origin + jnp.where(k == r, got[0:1, 1:2], 0.0)
    starts = starts + above + origin - down_first0

    lane = lax.broadcasted_iota(jnp.int32, (bands, LANES), 1)
    row_out[...] = jnp.where(
        lane == 0, row_total, jnp.where(lane == 1, starts + firsts[0], 0.0))
    copies = []
    for k in range(1, n_col):
        copies.append(pltpu.make_async_remote_copy(
            src_ref=row_out, dst_ref=row_in.at[k - 1],
            send_sem=row_send.at[k - 1], recv_sem=row_recv.at[k - 1],
            device_id=(r, lax.rem(c + k, n_col)), device_id_type=MESH))
    for copy in copies:
        copy.start()
    lax.fori_loop(bands // 2, bands, spectrum_step, 0)
    for copy in copies:
        copy.wait()
    offset = jnp.where(c == 0, starts + firsts[0], 0.0) - firsts[0]
    for k in range(1, n_col):
        got = row_in[k - 1]
        offset = offset + jnp.where(k <= c, got[:, 0:1], 0.0)
        offset = offset + jnp.where(k == c, got[:, 1:2], 0.0)
    for t in range(tiles):
        off_ref[:, t * TILE : (t + 1) * TILE] = jnp.broadcast_to(offset + along[t], (bands, TILE))
    for i in range(bands):
        band_copy(sh_s, high_hbm, high_sem, i).wait()
        band_copy(sl_s, low_hbm, low_sem, i).wait()


def per_device(n_row, n_col, x):
    height, width = x.shape
    bands = height // TILE
    cosine, inverse, weights = tables(TILE)
    high = cosine.astype(jnp.bfloat16)
    low = (cosine - high.astype(np.float32)).astype(jnp.bfloat16)
    beside, over = np.concatenate([high, low], 1), np.concatenate([high, low], 0)
    beside_t = np.concatenate([high.T, low.T], 1)
    over_t = np.concatenate([high.T, low.T], 0)
    w = np.zeros((TILE, 2 * TILE + LANES), np.float32)
    w[:, 0:TILE] = weights[0]
    w[:, TILE : 2 * TILE] = weights[1]
    w[:, 2 * TILE] = weights[0]
    w[:, 2 * TILE + 1] = weights[1]

    vmem = pl.BlockSpec(memory_space=pltpu.VMEM)
    anywhere = pl.BlockSpec(memory_space=pl.ANY)
    f32, bf16 = jnp.float32, jnp.bfloat16
    high_s, low_s, offsets = pl.pallas_call(
        functools.partial(chain_kernel, n_row, n_col),
        out_shape=[
            jax.ShapeDtypeStruct(x.shape, bf16),
            jax.ShapeDtypeStruct(x.shape, bf16),
            jax.ShapeDtypeStruct((bands, width), f32),
        ],
        in_specs=[anywhere] + [vmem] * 4,
        out_specs=[anywhere, anywhere, vmem],
        scratch_shapes=[
            pltpu.VMEM((height, width), f32),
            pltpu.VMEM((height, width), bf16),
            pltpu.VMEM((height, width), bf16),
            pltpu.VMEM((height, width), bf16),
            pltpu.VMEM((height, width), bf16),
            pltpu.VMEM((bands, TILE), f32),
            pltpu.VMEM((bands, TILE), f32),
            pltpu.VMEM((8, TILE), f32),
            pltpu.VMEM((8, TILE), f32),
            pltpu.VMEM((bands, width), f32),
            pltpu.VMEM((2 * bands, TILE), f32),
            pltpu.VMEM((bands, TILE), f32),
            pltpu.VMEM((2 * bands, TILE), f32),
            pltpu.VMEM((8, LANES), f32),
            pltpu.VMEM((n_row - 1, 8, LANES), f32),
            pltpu.VMEM((bands, LANES), f32),
            pltpu.VMEM((n_col - 1, bands, LANES), f32),
            pltpu.SemaphoreType.DMA((2,)),
            pltpu.SemaphoreType.DMA((2,)),
            pltpu.SemaphoreType.DMA((n_row - 1,)),
            pltpu.SemaphoreType.DMA((n_row - 1,)),
            pltpu.SemaphoreType.DMA((n_col - 1,)),
            pltpu.SemaphoreType.DMA((n_col - 1,)),
            pltpu.SemaphoreType.DMA((bands,)),
            pltpu.SemaphoreType.DMA((bands,)),
            pltpu.SemaphoreType.DMA((bands,)),
        ],
        compiler_params=pltpu.CompilerParams(collective_id=0, has_side_effects=True),
        name="chain",
    )(x, jnp.asarray(w), jnp.asarray(beside), jnp.asarray(over_t), jnp.asarray(inverse))

    return pl.pallas_call(
        finish_kernel,
        out_shape=jax.ShapeDtypeStruct(x.shape, f32),
        in_specs=[anywhere, anywhere, vmem, vmem, vmem],
        out_specs=anywhere,
        scratch_shapes=[
            pltpu.VMEM((height, width), bf16),
            pltpu.VMEM((height, width), bf16),
            pltpu.VMEM((height, width), f32),
            pltpu.SemaphoreType.DMA((bands,)),
            pltpu.SemaphoreType.DMA((bands,)),
            pltpu.SemaphoreType.DMA((bands,)),
        ],
        name="finish",
    )(high_s, low_s, offsets, jnp.asarray(beside_t), jnp.asarray(over))


def solution(mesh):
    n_row, n_col = mesh.shape["row"], mesh.shape["col"]
    return jax.shard_map(
        functools.partial(per_device, n_row, n_col), mesh=mesh,
        in_specs=(P("row", "col"),), out_specs=P("row", "col"), check_vma=False,
    )
```

```python
import functools
import math

import jax
import jax.numpy as jnp
import numpy as np
from jax import lax
from jax.experimental import pallas as pl
from jax.experimental.pallas import tpu as pltpu
from jax.sharding import PartitionSpec as P

TILE = 256
FULL_TURN = 2.0 * math.pi
MESH = pl.DeviceIdType.MESH
LANES = 128


def wrap_turns(values):
    return values - jnp.round(values)


def cos32(angle):
    return np.cos(angle.astype(np.float64)).astype(np.float32)


def tables(length):
    f32 = np.float32
    order = np.arange(length, dtype=f32)
    angle = (f32(math.pi) * order)[:, None] * (f32(2) * order + f32(1))[None, :] / f32(2 * length)
    cosine = cos32(angle) * f32(math.sqrt(2.0 / length))
    cosine[0] = cosine[0] * f32(math.sqrt(0.5))
    wave = f32(2) * cos32(f32(math.pi) * order / f32(length))
    eigen = (wave[:, None] + wave[None, :]) - f32(4)
    eigen[0, 0] = -1
    inverse = 1.0 / eigen.astype(np.float64)
    inverse[0, 0] = 0
    c64 = cosine.astype(np.float64)
    weights = []
    for cell in (length - 1, 0):
        green = (c64[:, cell] * inverse[0]) @ c64
        step = green - np.append(green[1:], 0.0)
        step[-1] = 0
        weights.append(step / length)
    return cosine, inverse.astype(f32), np.stack(weights).astype(f32)


def split(values):
    high = values.astype(jnp.bfloat16)
    low = (values - high.astype(jnp.float32)).astype(jnp.bfloat16)
    return high, low


def dot(left, right):
    return jnp.dot(left, right, preferred_element_type=jnp.float32)


def stack3(high, low, axis):
    return jnp.concatenate([high, low, high], axis)


BLOCKS = TILE // LANES


def wide(ref, first, rows):
    return jnp.concatenate([ref[first + l, rows, :] for l in range(BLOCKS)], 1)


def put_wide(ref, first, rows, values):
    for l in range(values.shape[1] // LANES):
        ref[first + l, rows, :] = values[:, l * LANES : (l + 1) * LANES]


def in_blocks(table):
    return np.ascontiguousarray(
        table.reshape(table.shape[0], -1, LANES).transpose(1, 0, 2))


def sandwich(high, low, right, left):
    first, second = pl.ds(0, TILE), pl.ds(TILE, TILE)
    table = [wide(right, 0, first), wide(right, 0, first), wide(right, 0, second)]
    inner = dot(stack3(high, low, 1), jnp.concatenate(table, 0))
    high, low = split(inner)
    table = [wide(left, 0, first), wide(left, 0, first), wide(left, BLOCKS, first)]
    return dot(jnp.concatenate(table, 1), stack3(high, low, 0))


def band_rows(i):
    return pl.ds(pl.multiple_of(i * TILE, TILE), TILE)


def band_copy(src, dst, sem, i):
    rows = band_rows(i)
    view = lambda ref: ref.at[rows, :] if len(ref.shape) == 2 else ref.at[:, rows, :]
    return pltpu.make_async_copy(view(src), view(dst), sem.at[i])


def finish_kernel(
    high_hbm, low_hbm, off_ref, left, right, out_hbm, high_s, low_s, out_s, high_sem, low_sem, out_sem
):
    height, width = out_s.shape
    bands, tiles = height // TILE, width // TILE
    for i in range(bands):
        band_copy(high_hbm, high_s, high_sem, i).start()
        band_copy(low_hbm, low_s, low_sem, i).start()

    def step(i, carry):
        rows = band_rows(i)
        band_copy(high_hbm, high_s, high_sem, i).wait()
        band_copy(low_hbm, low_s, low_sem, i).wait()
        for t in range(tiles):
            cols = slice(t * TILE, (t + 1) * TILE)
            high, low = wide(high_s, t * BLOCKS, rows), wide(low_s, t * BLOCKS, rows)
            solved = sandwich(high, low, right, left)
            out_s[rows, cols] = solved + off_ref[pl.ds(i, 1), cols]
        band_copy(out_s, out_hbm, out_sem, i).start()
        return carry

    lax.fori_loop(0, bands, step, 0)
    for i in range(bands):
        band_copy(out_s, out_hbm, out_sem, i).wait()


def lane_sum(values):
    return jnp.sum(values, axis=1, keepdims=True)


def running(values):
    n = values.shape[0]
    row = lax.broadcasted_iota(jnp.int32, values.shape, 0)
    total = jnp.zeros_like(values)
    for k in range(n - 1):
        total = total + jnp.where(row > k, values[k : k + 1], 0.0)
    return total


CHUNK = 32


def slope_band(x_s, w_ref, i, bands, dh_s, dl_s, sum_s, sum_d, first_s, last_s):
    width = x_s.shape[1]
    base = pl.multiple_of(i * TILE, TILE)
    shape = (CHUNK, width)
    row_id = lax.broadcasted_iota(jnp.int32, shape, 0)
    tile_end = lax.broadcasted_iota(jnp.int32, shape, 1) % TILE == TILE - 1
    fold = lambda v: jnp.sum(v.reshape(CHUNK // 8, 8, v.shape[1]), axis=0)
    acc = jnp.zeros((8, width), jnp.float32)
    acc_last = jnp.zeros((8, TILE), jnp.float32)
    acc_first = jnp.zeros((8, TILE), jnp.float32)
    before = jnp.zeros((1, width), jnp.float32)
    for k in range(TILE // CHUNK):
        rows = pl.ds(base + k * CHUNK, CHUNK)
        x = x_s[rows, :] * (1.0 / FULL_TURN)
        below = pltpu.roll(x, CHUNK - 1, 0)
        if k < TILE // CHUNK - 1:
            below = jnp.where(row_id == CHUNK - 1, x_s[pl.ds(base + (k + 1) * CHUNK, 1), :] * (1.0 / FULL_TURN), below)
        down = wrap_turns(below - x)
        if k == TILE // CHUNK - 1:
            down = jnp.where(row_id == CHUNK - 1, 0.0, down)
        across = wrap_turns(pltpu.roll(x, width - 1, 1) - x)
        acc = acc + fold(across)
        weight = w_ref[k * CHUNK : (k + 1) * CHUNK, 2 * TILE : 2 * TILE + 2]
        acc_last = acc_last + fold(down[:, :TILE] * weight[:, 0:1])
        acc_first = acc_first + fold(down[:, :TILE] * weight[:, 1:2])
        across = jnp.where(tile_end, 0.0, across)
        above = jnp.where(row_id == 0, before, pltpu.roll(down, 1, 0))
        before = down[CHUNK - 1 : CHUNK, :]
        high, low = split(down - above + across - pltpu.roll(across, 1, 1))
        put_wide(dh_s, 0, rows, high)
        put_wide(dl_s, 0, rows, low)
    sum_s[pl.ds(i, 1), :] = jnp.sum(acc, axis=0, keepdims=True)
    sum_d[pl.ds(i, 1), :] = jnp.sum(acc_last, axis=0, keepdims=True)
    sum_d[pl.ds(bands + i, 1), :] = jnp.sum(acc_first, axis=0, keepdims=True)
    first_s[pl.ds(i, 1), :] = x_s[pl.ds(base, 1), 0:TILE]
    last_s[pl.ds(i, 1), :] = x_s[pl.ds(base + TILE - 1, 1), 0:TILE]


def chain_kernel(
    n_row, n_col, x_hbm, w_ref, left, right, inv_ref, high_hbm, low_hbm, off_ref,
    x_s, dh_s, dl_s, sh_s, sl_s,
    col_out, col_in, top_out, top_in, sum_s, sum_d, first_s, last_s,
    down_out, down_in, row_out, row_in,
    edge_send, edge_recv, down_send, down_recv, row_send, row_recv,
    x_sem, high_sem, low_sem,
):
    r, c = lax.axis_index("row"), lax.axis_index("col")
    height, width = x_s.shape
    bands, tiles = height // TILE, width // TILE
    for i in range(bands):
        band_copy(x_hbm, x_s, x_sem, i).start()

    barrier = pltpu.get_barrier_semaphore()
    for k in range(1, n_row):
        pl.semaphore_signal(barrier, inc=1, device_id=(lax.rem(r + k, n_row), c), device_id_type=MESH)
    for k in range(1, n_col):
        pl.semaphore_signal(barrier, inc=1, device_id=(r, lax.rem(c + k, n_col)), device_id_type=MESH)

    def take_columns(i, carry):
        band_copy(x_hbm, x_s, x_sem, i).wait()
        rows = band_rows(i)
        col_out[pl.ds(i, 1), :] = jnp.transpose(x_s[rows, 0:LANES])[0:1, :]
        ends = jnp.transpose(x_s[rows, width - LANES : width])
        last_s[pl.ds(bands + i, 1), :] = ends[LANES - 1 : LANES, :]
        return carry

    lax.fori_loop(0, bands, take_columns, 0)
    top_out[...] = jnp.broadcast_to(x_s[0:1, 0:TILE], top_out.shape)

    pl.semaphore_wait(barrier, n_row + n_col - 2)
    edge_col = pltpu.make_async_remote_copy(
        src_ref=col_out, dst_ref=col_in, send_sem=edge_send.at[0], recv_sem=edge_recv.at[0],
        device_id=(r, lax.rem(c + n_col - 1, n_col)), device_id_type=MESH)
    edge_top = pltpu.make_async_remote_copy(
        src_ref=top_out, dst_ref=top_in, send_sem=edge_send.at[1], recv_sem=edge_recv.at[1],
        device_id=(lax.rem(r + n_row - 1, n_row), c), device_id_type=MESH)
    edge_col.start()
    edge_top.start()

    def slope_step(i, carry):
        slope_band(x_s, w_ref, i, bands, dh_s, dl_s, sum_s, sum_d, first_s, last_s)
        return carry

    lax.fori_loop(0, bands, slope_step, 0)

    def spectrum_step(i, carry):
        rows = band_rows(i)
        for t in range(tiles):
            high, low = wide(dh_s, t * BLOCKS, rows), wide(dl_s, t * BLOCKS, rows)
            high, low = split(sandwich(high, low, right, left) * inv_ref[...])
            put_wide(sh_s, t * BLOCKS, rows, high)
            put_wide(sl_s, t * BLOCKS, rows, low)
        band_copy(sh_s, high_hbm, high_sem, i).start()
        band_copy(sl_s, low_hbm, low_sem, i).start()
        return carry

    scale = FULL_TURN / TILE
    down_last = lane_sum(sum_d[0:bands, :])
    down_first = lane_sum(sum_d[bands : 2 * bands, :])
    edge_top.wait()
    edge_col.wait()
    below = jnp.concatenate([first_s[1:bands, :], top_in[0:1, :]], 0)
    border = lane_sum(wrap_turns((below - last_s[0:bands, :]) * (1.0 / FULL_TURN))) * scale
    band_id = lax.broadcasted_iota(jnp.int32, (bands, 1), 0)
    next_first = jnp.concatenate([down_first[1:bands], down_first[0:1]], 0)
    jump = down_last + border - next_first
    jump_total = jnp.sum(jump, axis=0, keepdims=True)
    starts = running(jump)
    lane = lax.broadcasted_iota(jnp.int32, (8, LANES), 1)
    down_first0 = down_first[0:1]
    down_out[...] = jnp.where(lane == 0, jump_total, jnp.where(lane == 1, down_first0, 0.0))
    copies = []
    for k in range(1, n_row):
        copies.append(pltpu.make_async_remote_copy(
            src_ref=down_out, dst_ref=down_in.at[k - 1],
            send_sem=down_send.at[k - 1], recv_sem=down_recv.at[k - 1],
            device_id=(lax.rem(r + k, n_row), c), device_id_type=MESH))
    for copy in copies:
        copy.start()

    sums = sum_s[...]
    last_w, first_w = w_ref[0:1, 0:TILE], w_ref[0:1, TILE : 2 * TILE]
    lasts = [lane_sum(sums[:, t * TILE : (t + 1) * TILE] * last_w) for t in range(tiles)]
    firsts = [lane_sum(sums[:, t * TILE : (t + 1) * TILE] * first_w) for t in range(tiles)]
    along = [jnp.zeros((bands, 1), jnp.float32)]
    for t in range(tiles - 1):
        end = (t + 1) * TILE
        along.append(along[-1] + lasts[t] + sums[:, end - 1 : end] * scale - firsts[t + 1])
    edge = lane_sum(wrap_turns((col_in[...] - last_s[bands : 2 * bands, :]) * (1.0 / FULL_TURN))) * scale
    row_total = along[-1] + lasts[-1] + edge - firsts[0]

    lax.fori_loop(0, bands // 2, spectrum_step, 0)
    for copy in copies:
        copy.wait()
    above = jnp.zeros((1, 1), jnp.float32)
    origin = jnp.where(r == 0, down_first0, 0.0)
    for k in range(1, n_row):
        got = down_in[k - 1]
        above = above + jnp.where(k <= r, got[0:1, 0:1], 0.0)
        origin = origin + jnp.where(k == r, got[0:1, 1:2], 0.0)
    starts = starts + above + origin - down_first0

    lane = lax.broadcasted_iota(jnp.int32, (bands, LANES), 1)
    row_out[...] = jnp.where(
        lane == 0, row_total, jnp.where(lane == 1, starts + firsts[0], 0.0))
    copies = []
    for k in range(1, n_col):
        copies.append(pltpu.make_async_remote_copy(
            src_ref=row_out, dst_ref=row_in.at[k - 1],
            send_sem=row_send.at[k - 1], recv_sem=row_recv.at[k - 1],
            device_id=(r, lax.rem(c + k, n_col)), device_id_type=MESH))
    for copy in copies:
        copy.start()
    lax.fori_loop(bands // 2, bands, spectrum_step, 0)
    for copy in copies:
        copy.wait()
    offset = jnp.where(c == 0, starts + firsts[0], 0.0) - firsts[0]
    for k in range(1, n_col):
        got = row_in[k - 1]
        offset = offset + jnp.where(k <= c, got[:, 0:1], 0.0)
        offset = offset + jnp.where(k == c, got[:, 1:2], 0.0)
    for t in range(tiles):
        off_ref[:, t * TILE : (t + 1) * TILE] = jnp.broadcast_to(offset + along[t], (bands, TILE))
    for i in range(bands):
        band_copy(sh_s, high_hbm, high_sem, i).wait()
        band_copy(sl_s, low_hbm, low_sem, i).wait()


def per_device(n_row, n_col, x):
    height, width = x.shape
    bands = height // TILE
    blocks = (width // LANES, height, LANES)
    cosine, inverse, weights = tables(TILE)
    high = cosine.astype(jnp.bfloat16)
    low = (cosine - high.astype(np.float32)).astype(jnp.bfloat16)
    beside = in_blocks(np.concatenate([high, low], 1))
    over = in_blocks(np.concatenate([high, low], 0))
    beside_t = in_blocks(np.concatenate([high.T, low.T], 1))
    over_t = in_blocks(np.concatenate([high.T, low.T], 0))
    w = np.zeros((TILE, 2 * TILE + LANES), np.float32)
    weights = weights * np.float32(FULL_TURN)
    w[:, 0:TILE] = weights[0]
    w[:, TILE : 2 * TILE] = weights[1]
    w[:, 2 * TILE] = weights[0]
    w[:, 2 * TILE + 1] = weights[1]

    vmem = pl.BlockSpec(memory_space=pltpu.VMEM)
    anywhere = pl.BlockSpec(memory_space=pl.ANY)
    f32, bf16 = jnp.float32, jnp.bfloat16
    high_s, low_s, offsets = pl.pallas_call(
        functools.partial(chain_kernel, n_row, n_col),
        out_shape=[
            jax.ShapeDtypeStruct(blocks, bf16),
            jax.ShapeDtypeStruct(blocks, bf16),
            jax.ShapeDtypeStruct((bands, width), f32),
        ],
        in_specs=[anywhere] + [vmem] * 4,
        out_specs=[anywhere, anywhere, vmem],
        scratch_shapes=[
            pltpu.VMEM((height, width), f32),
            pltpu.VMEM(blocks, bf16),
            pltpu.VMEM(blocks, bf16),
            pltpu.VMEM(blocks, bf16),
            pltpu.VMEM(blocks, bf16),
            pltpu.VMEM((bands, TILE), f32),
            pltpu.VMEM((bands, TILE), f32),
            pltpu.VMEM((8, TILE), f32),
            pltpu.VMEM((8, TILE), f32),
            pltpu.VMEM((bands, width), f32),
            pltpu.VMEM((2 * bands, TILE), f32),
            pltpu.VMEM((bands, TILE), f32),
            pltpu.VMEM((2 * bands, TILE), f32),
            pltpu.VMEM((8, LANES), f32),
            pltpu.VMEM((n_row - 1, 8, LANES), f32),
            pltpu.VMEM((bands, LANES), f32),
            pltpu.VMEM((n_col - 1, bands, LANES), f32),
            pltpu.SemaphoreType.DMA((2,)),
            pltpu.SemaphoreType.DMA((2,)),
            pltpu.SemaphoreType.DMA((n_row - 1,)),
            pltpu.SemaphoreType.DMA((n_row - 1,)),
            pltpu.SemaphoreType.DMA((n_col - 1,)),
            pltpu.SemaphoreType.DMA((n_col - 1,)),
            pltpu.SemaphoreType.DMA((bands,)),
            pltpu.SemaphoreType.DMA((bands,)),
            pltpu.SemaphoreType.DMA((bands,)),
        ],
        compiler_params=pltpu.CompilerParams(collective_id=0, has_side_effects=True),
        name="chain",
    )(x, jnp.asarray(w), jnp.asarray(beside), jnp.asarray(over_t), jnp.asarray(inverse * np.float32(FULL_TURN)))

    return pl.pallas_call(
        finish_kernel,
        out_shape=jax.ShapeDtypeStruct(x.shape, f32),
        in_specs=[anywhere, anywhere, vmem, vmem, vmem],
        out_specs=anywhere,
        scratch_shapes=[
            pltpu.VMEM(blocks, bf16),
            pltpu.VMEM(blocks, bf16),
            pltpu.VMEM((height, width), f32),
            pltpu.SemaphoreType.DMA((bands,)),
            pltpu.SemaphoreType.DMA((bands,)),
            pltpu.SemaphoreType.DMA((bands,)),
        ],
        name="finish",
    )(high_s, low_s, offsets, jnp.asarray(beside_t), jnp.asarray(over))


def solution(mesh):
    n_row, n_col = mesh.shape["row"], mesh.shape["col"]
    return jax.shard_map(
        functools.partial(per_device, n_row, n_col), mesh=mesh,
        in_specs=(P("row", "col"),), out_specs=P("row", "col"), check_vma=False,
    )
```

```python
import functools
import math

import jax
import jax.numpy as jnp
import numpy as np
from jax import lax
from jax.experimental import pallas as pl
from jax.experimental.pallas import tpu as pltpu
from jax.sharding import PartitionSpec as P

TILE = 256
FULL_TURN = 2.0 * math.pi
MESH = pl.DeviceIdType.MESH
LANES = 128


def wrap_turns(values):
    return values - jnp.round(values)


def cos32(angle):
    return np.cos(angle.astype(np.float64)).astype(np.float32)


def tables(length):
    f32 = np.float32
    order = np.arange(length, dtype=f32)
    angle = (f32(math.pi) * order)[:, None] * (f32(2) * order + f32(1))[None, :] / f32(2 * length)
    cosine = cos32(angle) * f32(math.sqrt(2.0 / length))
    cosine[0] = cosine[0] * f32(math.sqrt(0.5))
    wave = f32(2) * cos32(f32(math.pi) * order / f32(length))
    eigen = (wave[:, None] + wave[None, :]) - f32(4)
    eigen[0, 0] = -1
    inverse = 1.0 / eigen.astype(np.float64)
    inverse[0, 0] = 0
    c64 = cosine.astype(np.float64)
    weights = []
    for cell in (length - 1, 0):
        green = (c64[:, cell] * inverse[0]) @ c64
        step = green - np.append(green[1:], 0.0)
        step[-1] = 0
        weights.append(step / length)
    return cosine, inverse.astype(f32), np.stack(weights).astype(f32)


def split(values):
    high = values.astype(jnp.bfloat16)
    low = (values - high.astype(jnp.float32)).astype(jnp.bfloat16)
    return high, low


def dot(left, right):
    return jnp.dot(left, right, preferred_element_type=jnp.float32)


def stack3(high, low, axis):
    return jnp.concatenate([high, low, high], axis)


BLOCKS = TILE // LANES


def wide(ref, first, rows):
    return jnp.concatenate([ref[first + l, rows, :] for l in range(BLOCKS)], 1)


def put_wide(ref, first, rows, values):
    for l in range(values.shape[1] // LANES):
        ref[first + l, rows, :] = values[:, l * LANES : (l + 1) * LANES]


def in_blocks(table):
    return np.ascontiguousarray(
        table.reshape(table.shape[0], -1, LANES).transpose(1, 0, 2))


def sandwich(pairs, right, left):
    first, second = pl.ds(0, TILE), pl.ds(TILE, TILE)
    table = [wide(right, 0, first), wide(right, 0, first), wide(right, 0, second)]
    table = jnp.concatenate(table, 0)
    inner = [split(dot(stack3(high, low, 1), table)) for high, low in pairs]
    table = [wide(left, 0, first), wide(left, 0, first), wide(left, BLOCKS, first)]
    table = jnp.concatenate(table, 1)
    return [dot(table, stack3(high, low, 0)) for high, low in inner]


def group_size(bands, most):
    return next(g for g in range(most, 0, -1) if bands % g == 0)


def band_rows(i):
    return pl.ds(pl.multiple_of(i * TILE, TILE), TILE)


def band_copy(src, dst, sem, i):
    rows = band_rows(i)
    view = lambda ref: ref.at[rows, :] if len(ref.shape) == 2 else ref.at[:, rows, :]
    return pltpu.make_async_copy(view(src), view(dst), sem.at[i])


def finish_kernel(
    high_hbm, low_hbm, off_ref, left, right, out_hbm, high_s, low_s, out_s, high_sem, low_sem, out_sem
):
    height, width = out_s.shape
    bands, tiles = height // TILE, width // TILE
    for i in range(bands):
        band_copy(high_hbm, high_s, high_sem, i).start()
        band_copy(low_hbm, low_s, low_sem, i).start()

    group = group_size(bands, 2)

    def step(j, carry):
        some = [j * group + k for k in range(group)]
        for i in some:
            band_copy(high_hbm, high_s, high_sem, i).wait()
            band_copy(low_hbm, low_s, low_sem, i).wait()
        places = [(i, t) for i in some for t in range(tiles)]
        pairs = [
            (wide(high_s, t * BLOCKS, band_rows(i)), wide(low_s, t * BLOCKS, band_rows(i)))
            for i, t in places
        ]
        for (i, t), solved in zip(places, sandwich(pairs, right, left)):
            cols = slice(t * TILE, (t + 1) * TILE)
            out_s[band_rows(i), cols] = solved + off_ref[pl.ds(i, 1), cols]
        for i in some:
            band_copy(out_s, out_hbm, out_sem, i).start()
        return carry

    lax.fori_loop(0, bands // group, step, 0)
    for i in range(bands):
        band_copy(out_s, out_hbm, out_sem, i).wait()


def lane_sum(values):
    return jnp.sum(values, axis=1, keepdims=True)


def running(values):
    n = values.shape[0]
    row = lax.broadcasted_iota(jnp.int32, values.shape, 0)
    total = jnp.zeros_like(values)
    for k in range(n - 1):
        total = total + jnp.where(row > k, values[k : k + 1], 0.0)
    return total


CHUNK = 32


def slope_band(x_s, w_ref, i, bands, dh_s, dl_s, sum_s, sum_d, first_s, last_s):
    width = x_s.shape[1]
    base = pl.multiple_of(i * TILE, TILE)
    shape = (CHUNK, width)
    row_id = lax.broadcasted_iota(jnp.int32, shape, 0)
    tile_end = lax.broadcasted_iota(jnp.int32, shape, 1) % TILE == TILE - 1
    fold = lambda v: jnp.sum(v.reshape(CHUNK // 8, 8, v.shape[1]), axis=0)
    acc = jnp.zeros((8, width), jnp.float32)
    acc_last = jnp.zeros((8, TILE), jnp.float32)
    acc_first = jnp.zeros((8, TILE), jnp.float32)
    before = jnp.zeros((1, width), jnp.float32)
    for k in range(TILE // CHUNK):
        rows = pl.ds(base + k * CHUNK, CHUNK)
        x = x_s[rows, :] * (1.0 / FULL_TURN)
        below = pltpu.roll(x, CHUNK - 1, 0)
        if k < TILE // CHUNK - 1:
            below = jnp.where(row_id == CHUNK - 1, x_s[pl.ds(base + (k + 1) * CHUNK, 1), :] * (1.0 / FULL_TURN), below)
        down = wrap_turns(below - x)
        if k == TILE // CHUNK - 1:
            down = jnp.where(row_id == CHUNK - 1, 0.0, down)
        across = wrap_turns(pltpu.roll(x, width - 1, 1) - x)
        acc = acc + fold(across)
        weight = w_ref[k * CHUNK : (k + 1) * CHUNK, 2 * TILE : 2 * TILE + 2]
        acc_last = acc_last + fold(down[:, :TILE] * weight[:, 0:1])
        acc_first = acc_first + fold(down[:, :TILE] * weight[:, 1:2])
        across = jnp.where(tile_end, 0.0, across)
        above = jnp.where(row_id == 0, before, pltpu.roll(down, 1, 0))
        before = down[CHUNK - 1 : CHUNK, :]
        high, low = split(down - above + across - pltpu.roll(across, 1, 1))
        put_wide(dh_s, 0, rows, high)
        put_wide(dl_s, 0, rows, low)
    sum_s[pl.ds(i, 1), :] = jnp.sum(acc, axis=0, keepdims=True)
    sum_d[pl.ds(i, 1), :] = jnp.sum(acc_last, axis=0, keepdims=True)
    sum_d[pl.ds(bands + i, 1), :] = jnp.sum(acc_first, axis=0, keepdims=True)
    first_s[pl.ds(i, 1), :] = x_s[pl.ds(base, 1), 0:TILE]
    last_s[pl.ds(i, 1), :] = x_s[pl.ds(base + TILE - 1, 1), 0:TILE]


def chain_kernel(
    n_row, n_col, x_hbm, w_ref, left, right, inv_ref, high_hbm, low_hbm, off_ref,
    x_s, dh_s, dl_s, sh_s, sl_s,
    col_out, col_in, top_out, top_in, sum_s, sum_d, first_s, last_s,
    down_out, down_in, row_out, row_in,
    edge_send, edge_recv, down_send, down_recv, row_send, row_recv,
    x_sem, high_sem, low_sem,
):
    r, c = lax.axis_index("row"), lax.axis_index("col")
    height, width = x_s.shape
    bands, tiles = height // TILE, width // TILE
    for i in range(bands):
        band_copy(x_hbm, x_s, x_sem, i).start()

    barrier = pltpu.get_barrier_semaphore()
    for k in range(1, n_row):
        pl.semaphore_signal(barrier, inc=1, device_id=(lax.rem(r + k, n_row), c), device_id_type=MESH)
    for k in range(1, n_col):
        pl.semaphore_signal(barrier, inc=1, device_id=(r, lax.rem(c + k, n_col)), device_id_type=MESH)

    def take_columns(i, carry):
        band_copy(x_hbm, x_s, x_sem, i).wait()
        rows = band_rows(i)
        col_out[pl.ds(i, 1), :] = jnp.transpose(x_s[rows, 0:LANES])[0:1, :]
        ends = jnp.transpose(x_s[rows, width - LANES : width])
        last_s[pl.ds(bands + i, 1), :] = ends[LANES - 1 : LANES, :]
        return carry

    lax.fori_loop(0, bands, take_columns, 0)
    top_out[...] = jnp.broadcast_to(x_s[0:1, 0:TILE], top_out.shape)

    pl.semaphore_wait(barrier, n_row + n_col - 2)
    edge_col = pltpu.make_async_remote_copy(
        src_ref=col_out, dst_ref=col_in, send_sem=edge_send.at[0], recv_sem=edge_recv.at[0],
        device_id=(r, lax.rem(c + n_col - 1, n_col)), device_id_type=MESH)
    edge_top = pltpu.make_async_remote_copy(
        src_ref=top_out, dst_ref=top_in, send_sem=edge_send.at[1], recv_sem=edge_recv.at[1],
        device_id=(lax.rem(r + n_row - 1, n_row), c), device_id_type=MESH)
    edge_col.start()
    edge_top.start()

    def slope_step(i, carry):
        slope_band(x_s, w_ref, i, bands, dh_s, dl_s, sum_s, sum_d, first_s, last_s)
        return carry

    lax.fori_loop(0, bands, slope_step, 0)

    group = group_size(bands // 2, 4)

    def spectrum_step(j, carry):
        some = [j * group + k for k in range(group)]
        places = [(i, t) for i in some for t in range(tiles)]
        pairs = [
            (wide(dh_s, t * BLOCKS, band_rows(i)), wide(dl_s, t * BLOCKS, band_rows(i)))
            for i, t in places
        ]
        for (i, t), spectrum in zip(places, sandwich(pairs, right, left)):
            high, low = split(spectrum * inv_ref[...])
            put_wide(sh_s, t * BLOCKS, band_rows(i), high)
            put_wide(sl_s, t * BLOCKS, band_rows(i), low)
        for i in some:
            band_copy(sh_s, high_hbm, high_sem, i).start()
            band_copy(sl_s, low_hbm, low_sem, i).start()
        return carry

    scale = FULL_TURN / TILE
    down_last = lane_sum(sum_d[0:bands, :])
    down_first = lane_sum(sum_d[bands : 2 * bands, :])
    edge_top.wait()
    edge_col.wait()
    below = jnp.concatenate([first_s[1:bands, :], top_in[0:1, :]], 0)
    border = lane_sum(wrap_turns((below - last_s[0:bands, :]) * (1.0 / FULL_TURN))) * scale
    band_id = lax.broadcasted_iota(jnp.int32, (bands, 1), 0)
    next_first = jnp.concatenate([down_first[1:bands], down_first[0:1]], 0)
    jump = down_last + border - next_first
    jump_total = jnp.sum(jump, axis=0, keepdims=True)
    starts = running(jump)
    lane = lax.broadcasted_iota(jnp.int32, (8, LANES), 1)
    down_first0 = down_first[0:1]
    down_out[...] = jnp.where(lane == 0, jump_total, jnp.where(lane == 1, down_first0, 0.0))
    copies = []
    for k in range(1, n_row):
        copies.append(pltpu.make_async_remote_copy(
            src_ref=down_out, dst_ref=down_in.at[k - 1],
            send_sem=down_send.at[k - 1], recv_sem=down_recv.at[k - 1],
            device_id=(lax.rem(r + k, n_row), c), device_id_type=MESH))
    for copy in copies:
        copy.start()

    sums = sum_s[...]
    last_w, first_w = w_ref[0:1, 0:TILE], w_ref[0:1, TILE : 2 * TILE]
    lasts = [lane_sum(sums[:, t * TILE : (t + 1) * TILE] * last_w) for t in range(tiles)]
    firsts = [lane_sum(sums[:, t * TILE : (t + 1) * TILE] * first_w) for t in range(tiles)]
    along = [jnp.zeros((bands, 1), jnp.float32)]
    for t in range(tiles - 1):
        end = (t + 1) * TILE
        along.append(along[-1] + lasts[t] + sums[:, end - 1 : end] * scale - firsts[t + 1])
    edge = lane_sum(wrap_turns((col_in[...] - last_s[bands : 2 * bands, :]) * (1.0 / FULL_TURN))) * scale
    row_total = along[-1] + lasts[-1] + edge - firsts[0]

    half = bands // 2 // group
    lax.fori_loop(0, half, spectrum_step, 0)
    for copy in copies:
        copy.wait()
    above = jnp.zeros((1, 1), jnp.float32)
    origin = jnp.where(r == 0, down_first0, 0.0)
    for k in range(1, n_row):
        got = down_in[k - 1]
        above = above + jnp.where(k <= r, got[0:1, 0:1], 0.0)
        origin = origin + jnp.where(k == r, got[0:1, 1:2], 0.0)
    starts = starts + above + origin - down_first0

    lane = lax.broadcasted_iota(jnp.int32, (bands, LANES), 1)
    row_out[...] = jnp.where(
        lane == 0, row_total, jnp.where(lane == 1, starts + firsts[0], 0.0))
    copies = []
    for k in range(1, n_col):
        copies.append(pltpu.make_async_remote_copy(
            src_ref=row_out, dst_ref=row_in.at[k - 1],
            send_sem=row_send.at[k - 1], recv_sem=row_recv.at[k - 1],
            device_id=(r, lax.rem(c + k, n_col)), device_id_type=MESH))
    for copy in copies:
        copy.start()
    lax.fori_loop(half, bands // group, spectrum_step, 0)
    for copy in copies:
        copy.wait()
    offset = jnp.where(c == 0, starts + firsts[0], 0.0) - firsts[0]
    for k in range(1, n_col):
        got = row_in[k - 1]
        offset = offset + jnp.where(k <= c, got[:, 0:1], 0.0)
        offset = offset + jnp.where(k == c, got[:, 1:2], 0.0)
    for t in range(tiles):
        off_ref[:, t * TILE : (t + 1) * TILE] = jnp.broadcast_to(offset + along[t], (bands, TILE))
    for i in range(bands):
        band_copy(sh_s, high_hbm, high_sem, i).wait()
        band_copy(sl_s, low_hbm, low_sem, i).wait()


def per_device(n_row, n_col, x):
    height, width = x.shape
    bands = height // TILE
    blocks = (width // LANES, height, LANES)
    cosine, inverse, weights = tables(TILE)
    high = cosine.astype(jnp.bfloat16)
    low = (cosine - high.astype(np.float32)).astype(jnp.bfloat16)
    beside = in_blocks(np.concatenate([high, low], 1))
    over = in_blocks(np.concatenate([high, low], 0))
    beside_t = in_blocks(np.concatenate([high.T, low.T], 1))
    over_t = in_blocks(np.concatenate([high.T, low.T], 0))
    w = np.zeros((TILE, 2 * TILE + LANES), np.float32)
    weights = weights * np.float32(FULL_TURN)
    w[:, 0:TILE] = weights[0]
    w[:, TILE : 2 * TILE] = weights[1]
    w[:, 2 * TILE] = weights[0]
    w[:, 2 * TILE + 1] = weights[1]

    vmem = pl.BlockSpec(memory_space=pltpu.VMEM)
    anywhere = pl.BlockSpec(memory_space=pl.ANY)
    f32, bf16 = jnp.float32, jnp.bfloat16
    high_s, low_s, offsets = pl.pallas_call(
        functools.partial(chain_kernel, n_row, n_col),
        out_shape=[
            jax.ShapeDtypeStruct(blocks, bf16),
            jax.ShapeDtypeStruct(blocks, bf16),
            jax.ShapeDtypeStruct((bands, width), f32),
        ],
        in_specs=[anywhere] + [vmem] * 4,
        out_specs=[anywhere, anywhere, vmem],
        scratch_shapes=[
            pltpu.VMEM((height, width), f32),
            pltpu.VMEM(blocks, bf16),
            pltpu.VMEM(blocks, bf16),
            pltpu.VMEM(blocks, bf16),
            pltpu.VMEM(blocks, bf16),
            pltpu.VMEM((bands, TILE), f32),
            pltpu.VMEM((bands, TILE), f32),
            pltpu.VMEM((8, TILE), f32),
            pltpu.VMEM((8, TILE), f32),
            pltpu.VMEM((bands, width), f32),
            pltpu.VMEM((2 * bands, TILE), f32),
            pltpu.VMEM((bands, TILE), f32),
            pltpu.VMEM((2 * bands, TILE), f32),
            pltpu.VMEM((8, LANES), f32),
            pltpu.VMEM((n_row - 1, 8, LANES), f32),
            pltpu.VMEM((bands, LANES), f32),
            pltpu.VMEM((n_col - 1, bands, LANES), f32),
            pltpu.SemaphoreType.DMA((2,)),
            pltpu.SemaphoreType.DMA((2,)),
            pltpu.SemaphoreType.DMA((n_row - 1,)),
            pltpu.SemaphoreType.DMA((n_row - 1,)),
            pltpu.SemaphoreType.DMA((n_col - 1,)),
            pltpu.SemaphoreType.DMA((n_col - 1,)),
            pltpu.SemaphoreType.DMA((bands,)),
            pltpu.SemaphoreType.DMA((bands,)),
            pltpu.SemaphoreType.DMA((bands,)),
        ],
        compiler_params=pltpu.CompilerParams(collective_id=0, has_side_effects=True),
        name="chain",
    )(x, jnp.asarray(w), jnp.asarray(beside), jnp.asarray(over_t), jnp.asarray(inverse * np.float32(FULL_TURN)))

    return pl.pallas_call(
        finish_kernel,
        out_shape=jax.ShapeDtypeStruct(x.shape, f32),
        in_specs=[anywhere, anywhere, vmem, vmem, vmem],
        out_specs=anywhere,
        scratch_shapes=[
            pltpu.VMEM(blocks, bf16),
            pltpu.VMEM(blocks, bf16),
            pltpu.VMEM((height, width), f32),
            pltpu.SemaphoreType.DMA((bands,)),
            pltpu.SemaphoreType.DMA((bands,)),
            pltpu.SemaphoreType.DMA((bands,)),
        ],
        name="finish",
    )(high_s, low_s, offsets, jnp.asarray(beside_t), jnp.asarray(over))


def solution(mesh):
    n_row, n_col = mesh.shape["row"], mesh.shape["col"]
    return jax.shard_map(
        functools.partial(per_device, n_row, n_col), mesh=mesh,
        in_specs=(P("row", "col"),), out_specs=P("row", "col"), check_vma=False,
    )
```
